512 devices in a mesh: dp: 8 (over z_lo), row: 16 (over z_hi, x, core), col: 4 (over y).
Axes of the slice: x: 4, y: 4, z: 16 (z_hi: 2, z_lo: 8; z = z_hi * 8 + z_lo), core: 2. Of those that a mesh axis runs over, the one named last changes fastest.
Arguments:
- expand_gradient: bfloat16 [8, 4096, 5120], P('dp', 'row', 'col'), may hold values from -24 to 24, as said below
- expand_master: float32 [4096, 5120], P(('row', 'dp'), 'col'), may hold values from -0.12 to 0.12
- expand_rows: float32 [4096], P(('row', 'dp')), may hold values from 0.01 to 1
- expand_columns: float32 [5120], P('col'), may hold values from 0.01 to 1
- contract_gradient: bfloat16 [8, 5120, 4096], P('dp', 'row', 'col'), may hold values from -24 to 24, as said below
- contract_master: float32 [5120, 4096], P(('row', 'dp'), 'col'), may hold values from -0.12 to 0.12
- contract_rows: float32 [5120], P(('row', 'dp')), may hold values from 0.01 to 1
- contract_columns: float32 [4096], P('col'), may hold values from 0.01 to 1
- attend_gradient: bfloat16 [8, 4096, 4096], P('dp', 'row', 'col'), may hold values from -24 to 24, as said below
- attend_master: float32 [4096, 4096], P(('row', 'dp'), 'col'), may hold values from -0.12 to 0.12
- attend_rows: float32 [4096], P(('row', 'dp')), may hold values from 0.01 to 1
- attend_columns: float32 [4096], P('col'), may hold values from 0.01 to 1
Outputs:
- expand_updated: float32 [4096, 5120], P(('row', 'dp'), 'col')
- expand_weights: bfloat16 [4096, 5120], P('row', 'col')
- expand_rows_next: float32 [4096], P(('row', 'dp'))
- expand_columns_next: float32 [5120], P('col')
- expand_step: float32 [4096, 5120], P(('row', 'dp'), 'col')
- contract_updated: float32 [5120, 4096], P(('row', 'dp'), 'col')
- contract_weights: bfloat16 [5120, 4096], P('row', 'col')
- contract_rows_next: float32 [5120], P(('row', 'dp'))
- contract_columns_next: float32 [4096], P('col')
- contract_step: float32 [5120, 4096], P(('row', 'dp'), 'col')
- attend_updated: float32 [4096, 4096], P(('row', 'dp'), 'col')
- attend_weights: bfloat16 [4096, 4096], P('row', 'col')
- attend_rows_next: float32 [4096], P(('row', 'dp'))
- attend_columns_next: float32 [4096], P('col')
- attend_step: float32 [4096, 4096], P(('row', 'dp'), 'col')
The draws below stay inside these ranges and needn't reach their ends.
Inputs may be any that keep to these rules, and one draw needn't show every extreme that they name: `expand_gradient`: each replica's gradient, of any scale from entry to entry. `contract_gradient`: each replica's gradient, of any scale from entry to entry. `attend_gradient`: each replica's gradient, of any scale from entry to entry.
All inputs are finite; a program needn't handle non-finite values.
Results may differ from the reference program's by a relative error of at most 0.0004.
Values may be sent and summed in bfloat16 or wider, within the bound.
No kernel may reach another device: no remote copies, remote signals or barrier semaphores. Data moves between devices by JAX's collectives and lax.ppermute only.
A program may use at most 64 MiB of HBM per device.

```python
import math
import jax
import jax.numpy as jnp
from jax import lax

D = 4096
FF = 5120
INNER = 4096
REPLICAS = 8


def scale_field(key, height, width):
    row_pos = jnp.arange(height, dtype=jnp.float32) / height
    col_pos = jnp.arange(width, dtype=jnp.float32) / width
    logs = jnp.zeros((height, width), jnp.float32)
    for term in range(3):
        sub = jax.random.fold_in(key, 100 + term)
        freq_keys = jax.random.split(sub, 4)
        row_freq = jax.random.randint(freq_keys[0], (), 1, 5).astype(jnp.float32)
        col_freq = jax.random.randint(freq_keys[1], (), 1, 4).astype(jnp.float32)
        row_phase = jax.random.uniform(freq_keys[2], (), jnp.float32, 0.0, 2.0 * math.pi)
        col_phase = jax.random.uniform(freq_keys[3], (), jnp.float32, 0.0, 2.0 * math.pi)
        along_rows = jnp.cos(2.0 * math.pi * row_freq * row_pos + row_phase)
        along_cols = jnp.cos(2.0 * math.pi * col_freq * col_pos + col_phase)
        logs = logs + 0.6 * along_rows[:, None] * along_cols[None, :]
    return jnp.exp(logs)


def gradient_draw(key, replicas, height, width):
    field = scale_field(jax.random.fold_in(key, 7), height, width)
    noise_key = jax.random.fold_in(key, 11)
    noise = jax.random.normal(noise_key, (replicas, height, width), jnp.float32)
    values = jnp.clip(2.0 * noise * field[None, :, :], -24.0, 24.0)
    return values.astype(jnp.bfloat16)


def draw_expand_gradient(key, part):
    return gradient_draw(jax.random.fold_in(key, 1), REPLICAS, D, FF)


def draw_contract_gradient(key, part):
    return gradient_draw(jax.random.fold_in(key, 2), REPLICAS, FF, D)


def draw_attend_gradient(key, part):
    return gradient_draw(jax.random.fold_in(key, 3), REPLICAS, INNER, D)


def level_of(rng, shape, cuts, smallest, largest):
    factor_of = 1.0
    for position, parts in cuts:
        heights = jax.random.uniform(jax.random.fold_in(jax.random.fold_in(rng, 6), position), (parts,), jnp.float32, smallest / len(cuts), largest / len(cuts))
        factor_of = factor_of * jnp.repeat(jnp.exp(heights), shape[position] // parts).reshape((-1,) + (1,) * (len(shape) - 1 - position))
    return factor_of


def bell_draw(rng, extent, spread, limit, shards=(), held_as=jnp.bfloat16):
    values = spread * jax.random.normal(rng, extent, jnp.float32)
    if shards:
        values = values * level_of(rng, extent, shards, -0.22, 0.18)
    return jnp.clip(values, -limit, limit).astype(held_as)


def setup_inputs(seed: int = 0) -> dict:
    key_of = jax.random.split(jax.random.key(seed), 13)
    expand_gradient = draw_expand_gradient(jax.random.fold_in(key_of[12], 71), 0)
    expand_master = bell_draw(key_of[1], (D, FF), 0.02, 0.12, ((0, 128), (1, 4)), jnp.float32)
    expand_rows = jnp.clip(jnp.exp(math.log(1.0) - 4.6051702 * jax.random.uniform(key_of[2], (D,), jnp.float32) ** level_of(key_of[2], (D,), ((0, 128),), -0.2, 0.2)), 0.01, 1.0)
    expand_columns = jnp.clip(jnp.exp(math.log(1.0) - 4.6051702 * jax.random.uniform(key_of[3], (FF,), jnp.float32) ** level_of(key_of[3], (FF,), ((0, 4),), -0.2, 0.2)), 0.01, 1.0)
    contract_gradient = draw_contract_gradient(jax.random.fold_in(key_of[12], 71), 0)
    contract_master = bell_draw(key_of[5], (FF, D), 0.02, 0.12, ((0, 128), (1, 4)), jnp.float32)
    contract_rows = jnp.clip(jnp.exp(math.log(1.0) - 4.6051702 * jax.random.uniform(key_of[6], (FF,), jnp.float32) ** level_of(key_of[6], (FF,), ((0, 128),), -0.2, 0.2)), 0.01, 1.0)
    contract_columns = jnp.clip(jnp.exp(math.log(1.0) - 4.6051702 * jax.random.uniform(key_of[7], (D,), jnp.float32) ** level_of(key_of[7], (D,), ((0, 4),), -0.2, 0.2)), 0.01, 1.0)
    attend_gradient = draw_attend_gradient(jax.random.fold_in(key_of[12], 71), 0)
    attend_master = bell_draw(key_of[9], (INNER, D), 0.02, 0.12, ((0, 128), (1, 4)), jnp.float32)
    attend_rows = jnp.clip(jnp.exp(math.log(1.0) - 4.6051702 * jax.random.uniform(key_of[10], (INNER,), jnp.float32) ** level_of(key_of[10], (INNER,), ((0, 128),), -0.2, 0.2)), 0.01, 1.0)
    attend_columns = jnp.clip(jnp.exp(math.log(1.0) - 4.6051702 * jax.random.uniform(key_of[11], (D,), jnp.float32) ** level_of(key_of[11], (D,), ((0, 4),), -0.2, 0.2)), 0.01, 1.0)
    return dict(expand_gradient=expand_gradient, expand_master=expand_master, expand_rows=expand_rows, expand_columns=expand_columns, contract_gradient=contract_gradient, contract_master=contract_master, contract_rows=contract_rows, contract_columns=contract_columns, attend_gradient=attend_gradient, attend_master=attend_master, attend_rows=attend_rows, attend_columns=attend_columns)


def adapt(gradient, master, row_stat, column_stat):
    total = gradient[0].astype(jnp.float32)
    for which in range(1, gradient.shape[0]):
        total = total + gradient[which].astype(jnp.float32)
    mean_grad = total / gradient.shape[0]
    squares = mean_grad * mean_grad + 1e-30
    rows_next = 0.9 * row_stat + 0.1 * lax.optimization_barrier(jnp.mean(squares, axis=1))
    columns_next = 0.9 * column_stat + 0.1 * lax.optimization_barrier(jnp.mean(squares, axis=0))
    row_mean = jnp.mean(rows_next)
    update_raw = mean_grad * jnp.sqrt(row_mean / (rows_next[:, None] * columns_next[None, :]))
    clip_scale = jnp.maximum(1.0, jnp.sqrt(jnp.mean(update_raw * update_raw)))
    step_taken = update_raw / clip_scale
    updated = master - 0.01 * step_taken
    return (updated, updated.astype(jnp.bfloat16), rows_next, columns_next, step_taken)

def reference(expand_gradient, expand_master, expand_rows, expand_columns, contract_gradient, contract_master, contract_rows, contract_columns, attend_gradient, attend_master, attend_rows, attend_columns):
    first = adapt(expand_gradient, expand_master, expand_rows, expand_columns)
    second = adapt(contract_gradient, contract_master, contract_rows, contract_columns)
    third = adapt(attend_gradient, attend_master, attend_rows, attend_columns)
    return (first[0], first[1], first[2], first[3], first[4], second[0], second[1], second[2], second[3], second[4], third[0], third[1], third[2], third[3], third[4])
```

```python
import jax
import jax.numpy as jnp
from jax import lax
from jax.sharding import Mesh
from jax.sharding import PartitionSpec as P

ROW = ("row_0", "row_1", "row_2")
DP_ROW = ("dp", "row_0", "row_1", "row_2")
ROW_DP = ("row_0", "row_1", "row_2", "dp")


tiny_square = 1e-30
decay_rate = 0.9
learn_rate = 0.01
LANES = 128


def scatter_sum(gradient, me, count):
    blocks = gradient.reshape(count, gradient.shape[1] // count, gradient.shape[2])
    parts = [lax.dynamic_index_in_dim(blocks, me, 0, keepdims=False)]
    for s in range(1, count):
        block = lax.dynamic_index_in_dim(blocks, (me + s) % count, 0, keepdims=False)
        pairs = [(i, (i + s) % count) for i in range(count)]
        parts.append(lax.ppermute(block, "dp", pairs))
    total = parts[0].astype(jnp.float32)
    for part in parts[1:]:
        total = total + part.astype(jnp.float32)
    return total / count


def everyone(values, axes):
    count = lax.axis_size(axes)
    copies = jnp.broadcast_to(values, (count, *values.shape))
    return lax.all_to_all(copies, axes, split_axis=0, concat_axis=0, tiled=True)


def gather_line(shards, me, count):
    up = [(k, k + 1) for k in range(count - 1)]
    down = [(k + 1, k) for k in range(count - 1)]
    rising = list(shards)
    falling = list(shards)
    from_below = []
    from_above = []
    for _ in range(count - 1):
        rising = [lax.ppermute(x, "dp", up) for x in rising]
        falling = [lax.ppermute(x, "dp", down) for x in falling]
        from_below.append(rising)
        from_above.append(falling)
    gathered = []
    for which, shard in enumerate(shards):
        whole = jnp.zeros((count, *shard.shape), shard.dtype)
        whole = lax.dynamic_update_index_in_dim(whole, shard, me, 0)
        for s in range(count - 1):
            ahead = me + 1 + s
            block = jnp.where(ahead < count, from_above[s][which], from_below[count - 2 - s][which])
            whole = lax.dynamic_update_index_in_dim(whole, block, ahead % count, 0)
        gathered.append(whole.reshape(count * shard.shape[0], shard.shape[1]))
    return gathered


def body(
    expand_gradient,
    expand_master,
    expand_rows,
    expand_columns,
    contract_gradient,
    contract_master,
    contract_rows,
    contract_columns,
    attend_gradient,
    attend_master,
    attend_rows,
    attend_columns,
):
    gradients = (expand_gradient, contract_gradient, attend_gradient)
    masters = (expand_master, contract_master, attend_master)
    rows = (expand_rows, contract_rows, attend_rows)
    columns = (expand_columns, contract_columns, attend_columns)
    every = range(3)
    me = lax.axis_index("dp")
    member = lax.axis_index(DP_ROW)
    dp_count = lax.axis_size("dp")
    split_count = lax.axis_size(DP_ROW)
    col_count = lax.axis_size("col")

    means = [scatter_sum(g, me, dp_count) for g in gradients]
    heights = [g.shape[0] * split_count for g in means]
    widths = [g.shape[1] * col_count for g in means]

    squares = [g * g for g in means]
    row_parts = jnp.concatenate([jnp.sum(sq + tiny_square, axis=1) for sq in squares])
    row_totals = jnp.sum(everyone(row_parts, "col"), axis=0)
    rows_next = []
    start = 0
    for which in every:
        n = means[which].shape[0]
        rows_next.append(
            decay_rate * rows[which] + (1.0 - decay_rate) * row_totals[start : start + n] / widths[which]
        )
        start += n

    column_parts = [jnp.sum(sq + tiny_square, axis=0).reshape(-1, LANES) for sq in squares]
    scaled_parts = [
        jnp.sum(squares[which] / rows_next[which][:, None], axis=0).reshape(-1, LANES) for which in every
    ]
    row_sums = [jnp.broadcast_to(jnp.sum(rows_next[which]), (1, LANES)) for which in every]
    outgoing = jnp.concatenate(column_parts + scaled_parts + row_sums, axis=0).T
    incoming = jnp.sum(lax.all_to_all(outgoing, DP_ROW, split_axis=0, concat_axis=0, tiled=True), axis=0)

    counts = [c.shape[0] for c in column_parts]
    slots = sum(counts)
    old_columns = jnp.concatenate([c.reshape(-1, LANES) for c in columns], axis=0).T
    old_own = lax.dynamic_index_in_dim(old_columns, member, 0, keepdims=False)
    height_of = jnp.concatenate([jnp.full((counts[which],), 1.0 / heights[which], jnp.float32) for which in every])
    own_next = decay_rate * old_own + (1.0 - decay_rate) * (incoming[:slots] * height_of)
    shares = incoming[slots : 2 * slots] / own_next
    row_means = [incoming[2 * slots + which] / heights[which] for which in every]
    clip_parts = []
    start = 0
    for which in every:
        clip_parts.append(jnp.sum(shares[start : start + counts[which]], keepdims=True))
        start += counts[which]
    gathered = everyone(jnp.concatenate([own_next] + clip_parts), DP_ROW)
    clip_own = jnp.sum(gathered[:, slots:], axis=0)
    columns_wide = gathered[:, :slots].T
    columns_next = []
    start = 0
    for which in every:
        columns_next.append(columns_wide[start : start + counts[which]].reshape(-1))
        start += counts[which]

    clip_sums = jnp.sum(everyone(clip_own, "col"), axis=0)

    updated = []
    steps = []
    for which in every:
        clip_mean = clip_sums[which] * row_means[which] / (heights[which] * widths[which])
        clip_scale = jnp.maximum(1.0, jnp.sqrt(clip_mean))
        raw = means[which] * jnp.sqrt(
            row_means[which] / (rows_next[which][:, None] * columns_next[which][None, :])
        )
        steps.append(raw / clip_scale)
        updated.append(masters[which] - learn_rate * steps[which])
    weights = gather_line([u.astype(jnp.bfloat16) for u in updated], me, dp_count)
    outputs = []
    for which in every:
        outputs.extend(
            [updated[which], weights[which], rows_next[which], columns_next[which], steps[which]]
        )
    return tuple(outputs)


def solution(mesh):
    finer = Mesh(
        mesh.devices.reshape(mesh.shape["dp"], 2, 4, 2, mesh.shape["col"]),
        ("dp", "row_0", "row_1", "row_2", "col"),
    )
    one = (P("dp", ROW, "col"), P(ROW_DP, "col"), P(ROW_DP), P("col"))
    out = (P(ROW_DP, "col"), P(ROW, "col"), P(ROW_DP), P("col"), P(ROW_DP, "col"))
    return jax.shard_map(body, mesh=finer, in_specs=one * 3, out_specs=out * 3, check_vma=False)
```

```python
import jax
import jax.numpy as jnp
from jax import lax
from jax.experimental import pallas as pl
from jax.experimental.pallas import tpu as pltpu
from jax.sharding import Mesh
from jax.sharding import PartitionSpec as P

ROW = ("row_0", "row_1", "row_2")
DP_ROW = ("dp", "row_0", "row_1", "row_2")
ROW_DP = ("row_0", "row_1", "row_2", "dp")


tiny_square = 1e-30
decay_rate = 0.9
learn_rate = 0.01

MEMBERS = 128
LOW = 64
WIDE = 1024
COUNT = 8
MATRIX_ROWS = (32, 40, 32)
MATRIX_WIDTH = (1280, 1024, 1024)
ROW_START = (0, 32, 72)
ROW_END = 104
SLOT_START = (0, 10, 18)
SLOTS = 26
PACKED = 112
PIECES = (
    (0, 0, 0, 32, 1024, 0, 0),
    (0, 0, 1024, 8, 256, 32, 0),
    (0, 8, 1024, 8, 256, 32, 256),
    (0, 16, 1024, 8, 256, 32, 512),
    (0, 24, 1024, 8, 256, 32, 768),
    (1, 0, 0, 40, 1024, 40, 0),
    (2, 0, 0, 32, 1024, 80, 0),
)


def spec(space=pltpu.VMEM):
    return pl.BlockSpec(memory_space=space)


def call(kernel, outs, operands, name, scalar=False):
    specs = [spec(pltpu.SMEM) if scalar and i == 0 else spec() for i in range(len(operands))]
    return pl.pallas_call(
        kernel,
        out_shape=outs,
        in_specs=specs,
        out_specs=jax.tree.map(lambda _: spec(), outs),
        name=name,
        compiler_params=pltpu.CompilerParams(vmem_limit_bytes=12 * 1024 * 1024),
    )(*operands)


def pack_kernel(me_ref, expand_ref, contract_ref, attend_ref, *out_refs):
    sources = (expand_ref, contract_ref, attend_ref)
    for s in range(COUNT):
        block = lax.rem(me_ref[0] + s, COUNT)
        for which, r, c, n, m, pr, pc in PIECES:
            first = pl.multiple_of(block * MATRIX_ROWS[which] + r, 8)
            out_refs[s][pr : pr + n, pc : pc + m] = sources[which][0, pl.ds(first, n), c : c + m]


def sum_kernel(*refs):
    parts, (mean_ref, rows_ref) = refs[:COUNT], refs[COUNT:]
    total = parts[0][...].astype(jnp.float32)
    for part in parts[1:]:
        total = total + part[...].astype(jnp.float32)
    mean = total / COUNT
    mean_ref[...] = mean
    squares = mean * mean + tiny_square
    extra = [
        jnp.sum(squares[32:40, 256 * k : 256 * k + 256], axis=1, keepdims=True) for k in range(4)
    ]
    first = jnp.sum(squares[:32], axis=1, keepdims=True) + jnp.concatenate(extra, axis=0)
    rest = jnp.sum(squares[40:], axis=1, keepdims=True)
    for k in range(4):
        rows_ref[k, 0:32] = jnp.broadcast_to(first, (32, MEMBERS))
        rows_ref[k, 32:] = jnp.broadcast_to(rest, (72, MEMBERS))


def columns_of(block, slot):
    which = 0 if slot < SLOT_START[1] else 1 if slot < SLOT_START[2] else 2
    first = 128 * (slot - SLOT_START[which])
    found = []
    for matrix, r, c, n, m, pr, pc in PIECES:
        if matrix == which and c <= first < c + m:
            at = pc + first - c
            found.append((block[pr : pr + n, at : at + 128], ROW_START[which] + r, n))
    return found


def column_kernel(mean_ref, heard_ref, old_ref, out_ref, next_ref):
    heard = heard_ref[0] + heard_ref[1] + heard_ref[2] + heard_ref[3]
    pieces = []
    for which in range(3):
        at, n = ROW_START[which], MATRIX_ROWS[which]
        pieces.append(
            decay_rate * old_ref[at : at + n]
            + (1.0 - decay_rate) * (heard[at : at + n] / (4 * MATRIX_WIDTH[which]))
        )
    rows = jnp.concatenate(pieces, axis=0)
    next_ref[...] = rows
    inverse = 1.0 / rows
    mean = mean_ref[...]
    raw = mean * mean
    lines = []
    scaled = []
    for slot in range(SLOTS):
        one = 0.0
        two = 0.0
        for part, at, n in columns_of(raw, slot):
            one = one + jnp.sum(part + tiny_square, axis=0, keepdims=True)
            two = two + jnp.sum(part * inverse[at : at + n], axis=0, keepdims=True)
        lines.append(one)
        scaled.append(two)
    for which in range(3):
        at, n = ROW_START[which], MATRIX_ROWS[which]
        lines.append(jnp.sum(rows[at : at + n], axis=0, keepdims=True))
    blank = jnp.zeros((LOW - SLOTS - 3, MEMBERS), jnp.float32)
    tail = jnp.zeros((MEMBERS - LOW - SLOTS, MEMBERS), jnp.float32)
    out_ref[...] = jnp.concatenate(lines + [blank] + scaled + [tail], axis=0).T


def share_kernel(heard_ref, old_ref, height_ref, out_ref, row_mean_ref):
    total = jnp.sum(heard_ref[...], axis=0, keepdims=True)
    total = jnp.broadcast_to(total, (8, MEMBERS))
    lane = lax.broadcasted_iota(jnp.int32, (8, MEMBERS), 1)
    scaled = pltpu.roll(total, LOW, 1)
    own = decay_rate * old_ref[...] + (1.0 - decay_rate) * (total / height_ref[...])
    own = jnp.where(lane < SLOTS, own, 1.0)
    shares = jnp.where(lane < SLOTS, scaled / own, 0.0)
    message = jnp.where(lane < LOW, own, pltpu.roll(shares, LOW, 1))
    out_ref[...] = jnp.broadcast_to(message[0:1], (MEMBERS, MEMBERS))
    for which in range(3):
        height = MATRIX_ROWS[which] * MEMBERS
        total_rows = jnp.sum(jnp.where(lane == SLOTS + which, total, 0.0), axis=1, keepdims=True)
        row_mean_ref[8 * which : 8 * which + 8] = jnp.broadcast_to(total_rows / height, (8, MEMBERS))


def clip_kernel(heard_ref, columns_ref, out_ref):
    turned = heard_ref[...].T
    columns_ref[...] = turned[:32]
    totals = []
    for which in range(3):
        start = LOW + SLOT_START[which]
        end = LOW + (SLOT_START + (SLOTS,))[which + 1]
        line = jnp.sum(turned[start:end], axis=0, keepdims=True)
        total = jnp.sum(line, axis=1, keepdims=True)
        totals.append(jnp.broadcast_to(total, (1, MEMBERS)))
    message = jnp.concatenate(totals + [jnp.zeros((5, MEMBERS), jnp.float32)], axis=0)
    for k in range(4):
        out_ref[k] = message


def update_kernel(
    heard_ref, row_mean_ref, mean_ref, rows_ref, columns_ref, m0_ref, m1_ref, m2_ref,
    u0_ref, u1_ref, u2_ref, s0_ref, s1_ref, s2_ref, weights_ref,
):
    masters = (m0_ref, m1_ref, m2_ref)
    updated = (u0_ref, u1_ref, u2_ref)
    steps = (s0_ref, s1_ref, s2_ref)
    clip_sums = heard_ref[0] + heard_ref[1] + heard_ref[2] + heard_ref[3]
    row_mean = []
    clip = []
    for which in range(3):
        mean_of = row_mean_ref[8 * which : 8 * which + 1]
        size = MATRIX_ROWS[which] * MEMBERS * 4 * MATRIX_WIDTH[which]
        row_mean.append(mean_of)
        clip.append(jnp.maximum(1.0, jnp.sqrt(clip_sums[which : which + 1] * mean_of / size)))
    for which, r, c, n, m, pr, pc in PIECES:
        at = ROW_START[which] + r
        rows = rows_ref[at : at + n]
        for q in range(m // 128):
            slot = SLOT_START[which] + c // 128 + q
            left = c + 128 * q
            factor = jnp.sqrt(row_mean[which] / (rows * columns_ref[slot : slot + 1]))
            step = mean_ref[pr : pr + n, pc + 128 * q : pc + 128 * q + 128] * factor / clip[which]
            value = masters[which][r : r + n, left : left + 128] - learn_rate * step
            steps[which][r : r + n, left : left + 128] = step
            updated[which][r : r + n, left : left + 128] = value
            weights_ref[pr : pr + n, pc + 128 * q : pc + 128 * q + 128] = value.astype(jnp.bfloat16)


def gather_line(shard, me):
    up = [(k, k + 1) for k in range(COUNT - 1)]
    down = [(k + 1, k) for k in range(COUNT - 1)]
    rising = shard
    falling = shard
    from_below = []
    from_above = []
    for _ in range(COUNT - 1):
        rising = lax.ppermute(rising, "dp", up)
        falling = lax.ppermute(falling, "dp", down)
        from_below.append(rising)
        from_above.append(falling)
    whole = jnp.zeros((COUNT, *shard.shape), shard.dtype)
    whole = lax.dynamic_update_index_in_dim(whole, shard, me, 0)
    for s in range(COUNT - 1):
        ahead = me + 1 + s
        block = jnp.where(ahead < COUNT, from_above[s], from_below[COUNT - 2 - s])
        whole = lax.dynamic_update_index_in_dim(whole, block, ahead % COUNT, 0)
    return whole


def unpack_kernel(packed_ref, w0_ref, w1_ref, w2_ref):
    outs = (w0_ref, w1_ref, w2_ref)
    for block in range(COUNT):
        for which, r, c, n, m, pr, pc in PIECES:
            first = block * MATRIX_ROWS[which] + r
            outs[which][first : first + n, c : c + m] = packed_ref[block, pr : pr + n, pc : pc + m]


def body(*arguments):
    gradients, masters, rows, columns = (arguments[k::4] for k in range(4))
    f32 = jnp.float32
    bf16 = jnp.bfloat16
    me = lax.axis_index("dp")
    member = lax.axis_index(DP_ROW)

    block = jax.ShapeDtypeStruct((PACKED, WIDE), bf16)
    square = jax.ShapeDtypeStruct((MEMBERS, MEMBERS), f32)
    packed = call(
        pack_kernel, [block] * COUNT, (me.reshape(1).astype(jnp.int32), *gradients), "pack", scalar=True
    )
    old_rows = jnp.broadcast_to(jnp.concatenate(rows)[:, None], (ROW_END, MEMBERS))
    old_columns = jnp.concatenate([c.reshape(-1, MEMBERS) for c in columns], axis=0).T
    old_own = lax.dynamic_slice_in_dim(old_columns, member, 1, axis=0)
    old_own = jnp.pad(old_own, ((0, 0), (0, MEMBERS - SLOTS)))
    own, old_rows, old_own = lax.optimization_barrier((packed[0], old_rows, old_own))
    parts = [own]
    for s in range(1, COUNT):
        parts.append(lax.ppermute(packed[s], "dp", [(i, (i + s) % COUNT) for i in range(COUNT)]))
    mean, row_parts = call(
        sum_kernel,
        [jax.ShapeDtypeStruct((PACKED, WIDE), f32), jax.ShapeDtypeStruct((4, ROW_END, MEMBERS), f32)],
        parts,
        "sum",
    )

    heard = lax.all_to_all(row_parts, "col", split_axis=0, concat_axis=0, tiled=True)
    outgoing, rows_wide = call(
        column_kernel,
        [square, jax.ShapeDtypeStruct((ROW_END, MEMBERS), f32)],
        (mean, heard, old_rows),
        "columns",
    )

    incoming = lax.all_to_all(outgoing, DP_ROW, split_axis=0, concat_axis=0, tiled=True)
    heights = [float(MATRIX_ROWS[k] * MEMBERS) for k in range(3)]
    ends = SLOT_START[1:] + (SLOTS,)
    height = [heights[k] for k in range(3) for _ in range(ends[k] - SLOT_START[k])]
    height = jnp.asarray(height + [1.0] * (MEMBERS - SLOTS), f32)[None, :]
    message, row_mean = call(
        share_kernel,
        [square, jax.ShapeDtypeStruct((24, MEMBERS), f32)],
        (incoming, old_own, height),
        "shares",
    )
    gathered = lax.all_to_all(message, DP_ROW, split_axis=0, concat_axis=0, tiled=True)
    columns_wide, clip_parts = call(
        clip_kernel,
        [jax.ShapeDtypeStruct((32, MEMBERS), f32), jax.ShapeDtypeStruct((4, 8, MEMBERS), f32)],
        (gathered,),
        "clip",
    )
    clip_sums = lax.all_to_all(clip_parts, "col", split_axis=0, concat_axis=0, tiled=True)

    shapes = [jax.ShapeDtypeStruct(m.shape, f32) for m in masters]
    *fresh, shard = call(
        update_kernel,
        shapes + shapes + [block],
        (clip_sums, row_mean, mean, rows_wide, columns_wide, *masters),
        "update",
    )
    updated, steps = fresh[:3], fresh[3:]
    whole = gather_line(shard, me)
    weights = call(
        unpack_kernel,
        [jax.ShapeDtypeStruct((COUNT * m.shape[0], m.shape[1]), bf16) for m in masters],
        (whole,),
        "unpack",
    )
    outputs = []
    for which in range(3):
        at, n = ROW_START[which], MATRIX_ROWS[which]
        slot, end = SLOT_START[which], ends[which]
        outputs.extend(
            [
                updated[which],
                weights[which],
                rows_wide[at : at + n, 0],
                columns_wide[slot:end].reshape(-1),
                steps[which],
            ]
        )
    return tuple(outputs)


def solution(mesh):
    finer = Mesh(
        mesh.devices.reshape(mesh.shape["dp"], 2, 4, 2, mesh.shape["col"]),
        ("dp", "row_0", "row_1", "row_2", "col"),
    )
    one = (P("dp", ROW, "col"), P(ROW_DP, "col"), P(ROW_DP), P("col"))
    out = (P(ROW_DP, "col"), P(ROW, "col"), P(ROW_DP), P("col"), P(ROW_DP, "col"))
    return jax.shard_map(body, mesh=finer, in_specs=one * 3, out_specs=out * 3, check_vma=False)
```

```python
import jax
import jax.numpy as jnp
from jax import lax
from jax.experimental import pallas as pl
from jax.experimental.pallas import tpu as pltpu
from jax.sharding import Mesh
from jax.sharding import PartitionSpec as P

ROW = ("row_0", "row_1", "row_2")
DP_ROW = ("dp", "row_0", "row_1", "row_2")
ROW_DP = ("row_0", "row_1", "row_2", "dp")


tiny_square = 1e-30
decay_rate = 0.9
learn_rate = 0.01

LANES = 128
NEAR = ("row_1", "row_2")
LINE = ("dp", "row_0")
NEAR_COL = ("row_1", "row_2", "col")
OWNERS = 8
OWNED = 4
TOTALS = 28
WIDE = 1024
COUNT = 8
MATRIX_ROWS = (32, 40, 32)
MATRIX_WIDTH = (1280, 1024, 1024)
ROW_START = (0, 32, 72)
ROW_END = 104
SLOT_START = (0, 10, 18)
SLOTS = 26
SLOT_END = (10, 18, 26)
PACKED = 112
PIECES = (
    (0, 0, 0, 32, 1024, 0, 0),
    (0, 0, 1024, 8, 256, 32, 0),
    (0, 8, 1024, 8, 256, 32, 256),
    (0, 16, 1024, 8, 256, 32, 512),
    (0, 24, 1024, 8, 256, 32, 768),
    (1, 0, 0, 40, 1024, 40, 0),
    (2, 0, 0, 32, 1024, 80, 0),
)


def spec(space=pltpu.VMEM):
    return pl.BlockSpec(memory_space=space)


def call(kernel, outs, operands, name, spaces={}, **more):
    return pl.pallas_call(
        kernel,
        out_shape=outs,
        in_specs=[spec(spaces.get(i, pltpu.VMEM)) for i in range(len(operands))],
        out_specs=[spec() for _ in outs],
        name=name,
        compiler_params=pltpu.CompilerParams(vmem_limit_bytes=12 * 1024 * 1024),
        **more,
    )(*operands)


def pack_kernel(me_ref, expand_ref, contract_ref, attend_ref, *rest):
    out_refs, sems = rest[:COUNT], rest[COUNT]
    sources = (expand_ref, contract_ref, attend_ref)
    copies = []
    for s in range(COUNT):
        block = lax.rem(me_ref[0] + s, COUNT)
        for i, (which, r, c, n, m, pr, pc) in enumerate(PIECES):
            first = pl.multiple_of(block * MATRIX_ROWS[which] + r, 8)
            copies.append(
                pltpu.make_async_copy(
                    sources[which].at[0, pl.ds(first, n), pl.ds(c, m)],
                    out_refs[s].at[pl.ds(pr, n), pl.ds(pc, m)],
                    sems.at[s, i],
                )
            )
    for copy in copies:
        copy.start()
    for copy in copies:
        copy.wait()


def sum_kernel(*refs):
    parts, (mean_ref, rows_ref) = refs[:COUNT], refs[COUNT:]
    total = parts[0][...].astype(jnp.float32)
    for part in parts[1:]:
        total = total + part[...].astype(jnp.float32)
    mean = total / COUNT
    mean_ref[...] = mean
    squares = mean * mean + tiny_square
    extra = [
        jnp.sum(squares[32:40, 256 * k : 256 * k + 256], axis=1, keepdims=True) for k in range(4)
    ]
    first = jnp.sum(squares[:32], axis=1, keepdims=True) + jnp.concatenate(extra, axis=0)
    rest = jnp.sum(squares[40:], axis=1, keepdims=True)
    for k in range(4):
        rows_ref[k, 0:32] = jnp.broadcast_to(first, (32, LANES))
        rows_ref[k, 32:] = jnp.broadcast_to(rest, (72, LANES))


def columns_of(block, slot):
    which = 0 if slot < SLOT_START[1] else 1 if slot < SLOT_START[2] else 2
    first = 128 * (slot - SLOT_START[which])
    found = []
    for matrix, r, c, n, m, pr, pc in PIECES:
        if matrix == which and c <= first < c + m:
            at = pc + first - c
            found.append((block[pr : pr + n, at : at + 128], ROW_START[which] + r, n))
    return found


def column_kernel(mean_ref, heard_ref, old_ref, out_ref, next_ref):
    heard = heard_ref[0] + heard_ref[1] + heard_ref[2] + heard_ref[3]
    pieces = []
    for which in range(3):
        at, n = ROW_START[which], MATRIX_ROWS[which]
        pieces.append(
            decay_rate * old_ref[at : at + n]
            + (1.0 - decay_rate) * (heard[at : at + n] / (4 * MATRIX_WIDTH[which]))
        )
    rows = jnp.concatenate(pieces, axis=0)
    next_ref[...] = rows
    inverse = 1.0 / rows
    mean = mean_ref[...]
    raw = mean * mean
    lines = []
    scaled = []
    for slot in range(SLOTS):
        one = 0.0
        two = 0.0
        for part, at, n in columns_of(raw, slot):
            one = one + jnp.sum(part + tiny_square, axis=0, keepdims=True)
            two = two + jnp.sum(part * inverse[at : at + n], axis=0, keepdims=True)
        lines.append(one)
        scaled.append(two)
    blank = jnp.zeros((1, LANES), jnp.float32)
    lines += [blank] * (TOTALS - SLOTS)
    scaled += [blank] * (OWNERS * OWNED - SLOTS)
    for which in range(3):
        at, n = ROW_START[which], MATRIX_ROWS[which]
        lines.append(jnp.sum(rows[at : at + n], axis=0, keepdims=True))
    lines.append(blank)
    for owner in range(OWNERS):
        mine = slice(OWNED * owner, OWNED * owner + OWNED)
        out_ref[owner] = jnp.concatenate(lines[mine] + scaled[mine], axis=0)


def slice_kernel(heard_ref, out_ref):
    total = heard_ref[0]
    for k in range(1, OWNERS):
        total = total + heard_ref[k]
    for k in range(16):
        out_ref[k] = total


def share_kernel(heard_ref, old_ref, height_ref, real_ref, out_ref):
    total = heard_ref[0]
    for k in range(1, 16):
        total = total + heard_ref[k]
    sums = total[:OWNED]
    own = decay_rate * old_ref[...] + (1.0 - decay_rate) * (sums / height_ref[...])
    shares = total[OWNED:] / own
    message = jnp.concatenate([jnp.where(real_ref[...] > 0.0, own, sums), shares], axis=0)
    for k in range(32):
        out_ref[k] = message


def update_kernel(
    col_ref, heard_ref, mean_ref, rows_ref, m0_ref, m1_ref, m2_ref,
    u0_ref, u1_ref, u2_ref, s0_ref, s1_ref, s2_ref, columns_ref, weights_ref,
):
    masters = (m0_ref, m1_ref, m2_ref)
    updated = (u0_ref, u1_ref, u2_ref)
    steps = (s0_ref, s1_ref, s2_ref)
    col = col_ref[0]
    totals = heard_ref[4 * (TOTALS // OWNED) + col]
    for owner in range(OWNERS):
        columns_ref[OWNED * owner : OWNED * owner + OWNED] = heard_ref[4 * owner + col][:OWNED]
    row_mean = []
    clip = []
    for which in range(3):
        mean_of = totals[which : which + 1] / (MATRIX_ROWS[which] * LANES)
        size = MATRIX_ROWS[which] * LANES * 4 * MATRIX_WIDTH[which]
        line = 0.0
        for slot in range(SLOT_START[which], SLOT_END[which]):
            at = OWNED + slot % OWNED
            for k in range(4):
                line = line + heard_ref[4 * (slot // OWNED) + k][at : at + 1]
        clip_sum = jnp.sum(line, axis=1, keepdims=True)
        row_mean.append(mean_of)
        clip.append(jnp.maximum(1.0, jnp.sqrt(clip_sum * mean_of / size)))
    for which, r, c, n, m, pr, pc in PIECES:
        at = ROW_START[which] + r
        rows = rows_ref[at : at + n]
        for q in range(m // 128):
            slot = SLOT_START[which] + c // 128 + q
            left = c + 128 * q
            factor = jnp.sqrt(row_mean[which] / (rows * columns_ref[slot : slot + 1]))
            step = mean_ref[pr : pr + n, pc + 128 * q : pc + 128 * q + 128] * factor / clip[which]
            value = masters[which][r : r + n, left : left + 128] - learn_rate * step
            steps[which][r : r + n, left : left + 128] = step
            updated[which][r : r + n, left : left + 128] = value
            weights_ref[pr : pr + n, pc + 128 * q : pc + 128 * q + 128] = value.astype(jnp.bfloat16)


def gather_line(shard, me):
    up = [(k, k + 1) for k in range(COUNT - 1)]
    down = [(k + 1, k) for k in range(COUNT - 1)]
    rising = shard
    falling = shard
    from_below = []
    from_above = []
    for _ in range(COUNT - 1):
        rising = lax.ppermute(rising, "dp", up)
        falling = lax.ppermute(falling, "dp", down)
        from_below.append(rising)
        from_above.append(falling)
    whole = jnp.zeros((COUNT, *shard.shape), shard.dtype)
    whole = lax.dynamic_update_index_in_dim(whole, shard, me, 0)
    for s in range(COUNT - 1):
        ahead = me + 1 + s
        block = jnp.where(ahead < COUNT, from_above[s], from_below[COUNT - 2 - s])
        whole = lax.dynamic_update_index_in_dim(whole, block, ahead % COUNT, 0)
    return whole


def unpack_kernel(packed_ref, w0_ref, w1_ref, w2_ref):
    outs = (w0_ref, w1_ref, w2_ref)
    for block in range(COUNT):
        for which, r, c, n, m, pr, pc in PIECES:
            first = block * MATRIX_ROWS[which] + r
            outs[which][first : first + n, c : c + m] = packed_ref[block, pr : pr + n, pc : pc + m]


def body(*arguments):
    gradients, masters, rows, columns = (arguments[k::4] for k in range(4))
    f32 = jnp.float32
    bf16 = jnp.bfloat16
    me = lax.axis_index("dp").reshape(1).astype(jnp.int32)
    col = lax.axis_index("col").reshape(1).astype(jnp.int32)
    owner = lax.axis_index(NEAR)

    block = jax.ShapeDtypeStruct((PACKED, WIDE), bf16)
    in_place = {0: pltpu.SMEM, 1: pltpu.HBM, 2: pltpu.HBM, 3: pltpu.HBM}
    packed = call(
        pack_kernel,
        [block] * COUNT,
        (me, *gradients),
        "pack",
        in_place,
        scratch_shapes=[pltpu.SemaphoreType.DMA((COUNT, len(PIECES)))],
    )
    slots = OWNERS * OWNED
    old_rows = jnp.broadcast_to(jnp.concatenate(rows)[:, None], (ROW_END, LANES))
    old_columns = jnp.concatenate([c.reshape(-1, LANES) for c in columns], axis=0)
    old_columns = jnp.pad(old_columns, ((0, slots - SLOTS), (0, 0)), constant_values=1.0)
    height_of = [1.0] * slots
    for which in range(3):
        for slot in range(SLOT_START[which], SLOT_END[which]):
            height_of[slot] = float(MATRIX_ROWS[which] * LANES)
    heights = jnp.broadcast_to(jnp.asarray(height_of, f32)[:, None], (slots, LANES))
    real = jnp.where(heights > 1.0, 1.0, 0.0)
    fixed = [lax.dynamic_slice_in_dim(x, OWNED * owner, OWNED, 0) for x in (old_columns, heights, real)]
    own, old_rows, *fixed = lax.optimization_barrier((packed[0], old_rows, *fixed))

    parts = [own]
    for s in range(1, COUNT):
        parts.append(lax.ppermute(packed[s], "dp", [(i, (i + s) % COUNT) for i in range(COUNT)]))
    mean, row_parts = call(
        sum_kernel,
        [jax.ShapeDtypeStruct((PACKED, WIDE), f32), jax.ShapeDtypeStruct((4, ROW_END, LANES), f32)],
        parts,
        "sum",
    )

    def exchange(messages, axes):
        return lax.all_to_all(messages, axes, split_axis=0, concat_axis=0, tiled=True)

    def tiles(count):
        return [jax.ShapeDtypeStruct((count, 8, LANES), f32)]

    heard = exchange(row_parts, "col")
    outgoing, rows_wide = call(
        column_kernel,
        tiles(OWNERS) + [jax.ShapeDtypeStruct((ROW_END, LANES), f32)],
        (mean, heard, old_rows),
        "columns",
    )
    (slices,) = call(slice_kernel, tiles(16), (exchange(outgoing, NEAR),), "slices")
    (message,) = call(share_kernel, tiles(32), (exchange(slices, LINE), *fixed), "shares")
    heard = exchange(message, NEAR_COL)

    shapes = [jax.ShapeDtypeStruct(m.shape, f32) for m in masters]
    *fresh, columns_wide, shard = call(
        update_kernel,
        shapes + shapes + [jax.ShapeDtypeStruct((slots, LANES), f32), block],
        (col, heard, mean, rows_wide, *masters),
        "update",
        {0: pltpu.SMEM},
    )
    updated, steps = fresh[:3], fresh[3:]
    whole = gather_line(shard, me[0])
    weights = call(
        unpack_kernel,
        [jax.ShapeDtypeStruct((COUNT * m.shape[0], m.shape[1]), bf16) for m in masters],
        (whole,),
        "unpack",
    )
    outputs = []
    for which in range(3):
        at, n = ROW_START[which], MATRIX_ROWS[which]
        slot, end = SLOT_START[which], SLOT_END[which]
        outputs.extend(
            [
                updated[which],
                weights[which],
                rows_wide[at : at + n, 0],
                columns_wide[slot:end].reshape(-1),
                steps[which],
            ]
        )
    return tuple(outputs)


def solution(mesh):
    finer = Mesh(
        mesh.devices.reshape(mesh.shape["dp"], 2, 4, 2, mesh.shape["col"]),
        ("dp", "row_0", "row_1", "row_2", "col"),
    )
    one = (P("dp", ROW, "col"), P(ROW_DP, "col"), P(ROW_DP), P("col"))
    out = (P(ROW_DP, "col"), P(ROW, "col"), P(ROW_DP), P("col"), P(ROW_DP, "col"))
    return jax.shard_map(body, mesh=finer, in_specs=one * 3, out_specs=out * 3, check_vma=False)
```
